128 devices in a mesh: vocab: 16 (over x, y), hid: 8 (over z, core).
Axes of the slice: x: 4, y: 4, z: 4, core: 2. Of those that a mesh axis runs over, the one named last changes fastest.
Arguments:
- hidden: bfloat16 [2, 512, 7168], P(None, 'vocab', 'hid'), may hold values from -100 to 100
- head_weight: bfloat16 [7168, 131072], P('hid', 'vocab'), may hold values from -2 to 2
- targets: int32 [2, 512], P(None, 'hid'), may hold values from 0 to 131071
Outputs:
- entropy: float32 [2, 512], P(None, 'hid')
- squared: float32 [2, 512], P(None, 'hid')
The draws below stay inside these ranges and needn't reach their ends.
All inputs are finite; a program needn't handle non-finite values.
Results may differ from the reference program's by a relative error of at most 0.0003.
Values may be sent and summed in bfloat16 or wider, within the bound.
No kernel may reach another device: no remote copies, remote signals or barrier semaphores. Data moves between devices by JAX's collectives and lax.ppermute only.
A program may use at most 192 MiB of HBM per device.

```python
import math
import jax
import jax.numpy as jnp

D = 7168
DEPTH = 2
VOCAB = 131072
TOKENS = 512


def column_block(key, index):
    block_key = jax.random.fold_in(jax.random.fold_in(key, 7001), index)
    column_ids = index * 128 + jnp.arange(128)
    column_ramp = 1.0 + 0.25 * column_ids.astype(jnp.float32) / VOCAB
    raw_values = jnp.clip(jax.random.normal(block_key, (D, 128), jnp.float32), -6.0, 6.0)
    return raw_values * column_ramp[None, :] / math.sqrt(D)


def draw_head_weight(key, part):
    blocks = jax.vmap(lambda index: column_block(key, index))(jnp.arange(VOCAB // 128))
    return jnp.transpose(blocks, (1, 0, 2)).reshape(D, VOCAB).astype(jnp.bfloat16)


def draw_hidden(key, part):
    hidden_key = jax.random.fold_in(key, 7002)
    base_values = 3.0 * jnp.clip(jax.random.normal(hidden_key, (DEPTH, TOKENS, D), jnp.float32), -6.0, 6.0)
    return jnp.clip(base_values, -100.0, 100.0).astype(jnp.bfloat16)


def touch_ends(result, rng, smallest, high):
    longest = result.shape.index(max(result.shape))
    spots = []
    for shift in (0, 1):
        where = [jax.random.randint(jax.random.fold_in(rng, axis), (), 0, length) for axis, length in enumerate(result.shape)]
        where[longest] = (where[longest] + shift) % result.shape[longest]
        spots.append(tuple(where))
    return result.at[spots[0]].set(smallest).at[spots[1]].set(high)


def setup_inputs(seed: int = 0) -> dict:
    key_of = jax.random.split(jax.random.key(seed), 4)
    hidden = draw_hidden(jax.random.fold_in(key_of[3], 71), 0)
    head_weight = draw_head_weight(jax.random.fold_in(key_of[3], 71), 0)
    targets = touch_ends(jax.random.randint(key_of[2], (DEPTH, TOKENS), 0, VOCAB), jax.random.fold_in(key_of[2], 1), 0, VOCAB - 1).astype(jnp.int32)
    return dict(hidden=hidden, head_weight=head_weight, targets=targets)


def reference(hidden, head_weight, targets):
    entropy_rows = []
    square_rows = []
    for depth_index in range(DEPTH):
        logits = jnp.dot(hidden[depth_index], head_weight, preferred_element_type=jnp.float32)
        row_peak = jnp.max(logits, axis=1)
        row_total = jnp.sum(jnp.exp(logits - row_peak[:, None]), axis=1)
        log_norm = row_peak + jnp.log(row_total)
        picked = jnp.take_along_axis(logits, targets[depth_index][:, None], axis=1)[:, 0]
        entropy_rows.append(log_norm - picked)
        square_rows.append(log_norm * log_norm)
    return jnp.stack(entropy_rows), jnp.stack(square_rows)
```

```python
import jax
import jax.numpy as jnp
from jax import lax
from jax.sharding import Mesh
from jax.sharding import PartitionSpec as P

VOCAB = ("vocab_0", "vocab_1")
HID = ("hid_0", "hid_1")
PLANE = ("vocab_0", "vocab_1", "hid_1")
RING = "hid_0"
CORE = "hid_1"
UP = [(i, (i + 1) % 4) for i in range(4)]
DOWN = [(i, (i - 1) % 4) for i in range(4)]
SWAP = [(0, 1), (1, 0)]
SCALE = 1.0 / 16.0


def packed(partial):
    return (partial * SCALE).astype(jnp.float16)


def unpacked(message):
    return message.astype(jnp.float32) * (1.0 / SCALE)


def dot(rows, columns):
    return jnp.dot(rows, columns, preferred_element_type=jnp.float32)


def body(hidden, head_weight, targets):
    ring = lax.axis_index(RING)
    core = lax.axis_index(CORE)
    vocab_index = lax.axis_index(VOCAB)
    width = head_weight.shape[1]
    half = width // 2
    other_weight = lax.ppermute(head_weight, CORE, SWAP)

    given = lax.dynamic_index_in_dim(targets, 1 - core, 0, False)
    kept = lax.dynamic_index_in_dim(targets, core, 0, False)
    found = lax.ppermute(given, CORE, SWAP)
    labels = jnp.where(
        core == 0, jnp.concatenate([kept, found]), jnp.concatenate([found, kept])
    )

    block = hidden.shape[1]
    sent = jnp.broadcast_to(hidden, (16, *hidden.shape)).reshape(32, *hidden.shape[1:])
    rows = lax.all_to_all(sent, PLANE, split_axis=0, concat_axis=0, tiled=True)
    rows = rows.reshape(4, 4, 2, block, hidden.shape[2])

    def part(step, which):
        piece = lax.dynamic_index_in_dim(rows, (ring + step) % 4, 0, False)
        piece = lax.dynamic_index_in_dim(piece, which, 1, False)
        return piece.reshape(4 * block, hidden.shape[2])

    def partial(step, lo):
        mine, theirs = part(step, core), part(step, 1 - core)
        return dot(mine, head_weight[:, lo : lo + half]) + dot(
            theirs, other_weight[:, lo : lo + half]
        )

    far_up = lax.ppermute(packed(partial(2, 0)), RING, UP)
    far_down = lax.ppermute(packed(partial(2, half)), RING, DOWN)
    near_up = lax.ppermute(packed(partial(1, half)), RING, UP)
    near_down = lax.ppermute(packed(partial(3, 0)), RING, DOWN)
    sum_up = lax.ppermute(packed(partial(1, 0) + unpacked(far_up)), RING, UP)
    sum_down = lax.ppermute(packed(partial(3, half) + unpacked(far_down)), RING, DOWN)
    low = partial(0, 0) + unpacked(near_down)
    high = partial(0, half) + unpacked(near_up)
    low, high = lax.optimization_barrier((low, high))
    low = low + unpacked(sum_up)
    high = high + unpacked(sum_down)

    first = vocab_index * width
    ids = first + lax.broadcasted_iota(jnp.int32, low.shape, 1)
    peak = jnp.maximum(jnp.max(low, axis=1), jnp.max(high, axis=1))
    mass = jnp.sum(jnp.exp(low - peak[:, None]), axis=1) + jnp.sum(
        jnp.exp(high - peak[:, None]), axis=1
    )
    picked = jnp.sum(jnp.where(ids == labels[:, None], low, 0.0), axis=1) + jnp.sum(
        jnp.where(ids + half == labels[:, None], high, 0.0), axis=1
    )

    stats = jnp.stack([peak, mass, picked])
    stats = stats.reshape(3, 2, -1).transpose(1, 0, 2)
    stats = jnp.broadcast_to(stats, (16, *stats.shape)).reshape(32, *stats.shape[1:])
    stats = lax.all_to_all(stats, PLANE, split_axis=0, concat_axis=0, tiled=True)
    stats = stats.reshape(16, 2, *stats.shape[1:])
    peaks, masses, picks = stats[:, :, 0], stats[:, :, 1], stats[:, :, 2]
    top = jnp.max(peaks, axis=0)
    total = jnp.sum(masses * jnp.exp(peaks - top), axis=0)
    log_norm = top + jnp.log(total)
    return log_norm - jnp.sum(picks, axis=0), log_norm * log_norm


def solution(mesh):
    finer = Mesh(mesh.devices.reshape(4, 4, 4, 2), (*VOCAB, *HID))
    return jax.shard_map(
        body,
        mesh=finer,
        in_specs=(P(None, VOCAB, HID), P(HID, VOCAB), P(None, HID)),
        out_specs=(P(None, HID), P(None, HID)),
        check_vma=False,
    )
```

```python
import jax
import jax.numpy as jnp
from jax import lax
from jax.experimental import pallas as pl
from jax.experimental.pallas import tpu as pltpu
from jax.sharding import Mesh
from jax.sharding import PartitionSpec as P

VOCAB = ("vocab_0", "vocab_1")
HID = ("hid_0", "hid_1")
EVERY = (*VOCAB, *HID)
RING = "hid_0"
CORE = "hid_1"
UP = [(i, (i + 1) % 4) for i in range(4)]
DOWN = [(i, (i - 1) % 4) for i in range(4)]
ACROSS = [(i, (i + 2) % 4) for i in range(4)]
SWAP = [(0, 1), (1, 0)]
WAYS = (UP, DOWN, ACROSS)
OFFSETS = (0, 3, 1, 2)
SCALE = 1.0 / 16.0


def packed(partial):
    return (partial * SCALE).astype(jnp.float16)


def unpacked(message):
    return message.astype(jnp.float32) * (1.0 / SCALE)


def dot(rows, columns):
    return jnp.dot(rows, columns, preferred_element_type=jnp.float32)


def after(value, *earlier):
    return lax.optimization_barrier((value, *earlier))[0]


def take(array, index, axis):
    return lax.dynamic_index_in_dim(array, index, axis, False)


def offset(k):
    return jnp.where(k == 0, 0, jnp.where(k == 1, 3, k - 1))


def fetch(given, kept, done):
    copy = pltpu.make_async_copy(given, kept, done)
    copy.start()
    copy.wait()


def resident(array):
    return pl.pallas_call(
        fetch,
        out_shape=pltpu.VMEM(array.shape, array.dtype),
        in_specs=[pl.BlockSpec(memory_space=pltpu.HBM)],
        out_specs=pl.BlockSpec(memory_space=pltpu.VMEM),
        scratch_shapes=[pltpu.SemaphoreType.DMA],
        compiler_params=pltpu.CompilerParams(vmem_limit_bytes=40 << 20),
        name="resident",
    )(array)


def losses(hidden, head_weight, targets):
    ring = lax.axis_index(RING)
    core = lax.axis_index(CORE)
    vocab_index = lax.axis_index(VOCAB)
    width = head_weight.shape[1]
    half = width // 2
    deal = hidden.shape[1] // 4
    weight = resident(head_weight)

    dealt = hidden.reshape(2, 4, deal, hidden.shape[2])
    dealt = jnp.stack([take(dealt, 1 - core, 0), take(dealt, core, 0)])
    dealt = jnp.stack([take(dealt, (ring + k) % 4, 1) for k in (2, 1, 3, 0)], axis=1)

    def token_of(row):
        plane_at = lax.rem(lax.axis_index(VOCAB[0]) + offset(row // (4 * deal)), 4)
        line_at = lax.rem(lax.axis_index(VOCAB[1]) + offset(row // deal % 4), 4)
        return 4 * deal * (4 * plane_at + line_at) + deal * ring + row % deal

    mine = lax.dynamic_slice_in_dim(targets, core, 1)
    mate = lax.dynamic_slice_in_dim(targets, 1 - core, 1)
    pair = jnp.concatenate([mine, lax.ppermute(mate, CORE, SWAP)])
    labels = 0
    for k, way in enumerate((None, *WAYS)):
        piece = pair if way is None else lax.ppermute(pair, RING, way)
        shape = (16 * deal, *piece.shape)
        side, place = (lax.broadcasted_iota(jnp.int32, shape, d) for d in (1, 2))
        owner = 2 * lax.rem(ring + OFFSETS[k], 4) + jnp.where(side == 0, core, 1 - core)
        wanted = token_of(lax.broadcasted_iota(jnp.int32, shape, 0))
        hit = owner * piece.shape[1] + place == wanted
        labels = labels + jnp.sum(jnp.where(hit, piece, 0), axis=(1, 2))

    def around(block, axis):
        return [lax.ppermute(block, axis, way) for way in WAYS]

    plane = [dealt, *around(dealt, VOCAB[1])]
    plane = jnp.stack(plane, axis=2).reshape(2, 4, 4 * deal, hidden.shape[2])
    far = around(plane[:, 0], VOCAB[0])
    rest = around(after(plane[:, 1:], labels), VOCAB[0])

    def given(rows, lo, size):
        partial = dot(rows[0], weight[:, lo : lo + size])
        return lax.ppermute(partial, CORE, SWAP)

    def both(rows, lo):
        found = given(rows, lo, half)
        return found + dot(rows[1], weight[:, lo : lo + half])

    first_far = plane[:, 0]
    found = given(first_far, 0, width)
    first_up = packed(found[:, :half] + dot(first_far[1], weight[:, :half]))
    first_down = packed(found[:, half:] + dot(first_far[1], weight[:, half:]))
    far = after(jnp.concatenate(far, axis=1), first_up, first_down)
    far_up = packed(both(far, 0))
    far_down = packed(both(far, half))
    rest = jnp.concatenate([plane[:, 1:], *rest], axis=2)
    rest = after(rest, far_up, far_down)
    near_up = packed(both(rest[:, 0], half))
    near_down = packed(both(rest[:, 1], 0))
    rest = after(rest, near_up, near_down)
    sum_low = both(rest[:, 0], 0)
    sum_high = both(rest[:, 1], half)
    own = after(rest, sum_low, sum_high)[:, 2]
    first_up = lax.ppermute(first_up, RING, UP)
    first_down = lax.ppermute(first_down, RING, DOWN)
    far_up = lax.ppermute(far_up, RING, UP)
    far_down = lax.ppermute(far_down, RING, DOWN)
    near_up = lax.ppermute(near_up, RING, UP)
    near_down = lax.ppermute(near_down, RING, DOWN)
    sum_low, sum_high = lax.optimization_barrier((sum_low, sum_high))
    far_up = jnp.concatenate([first_up, far_up])
    far_down = jnp.concatenate([first_down, far_down])
    sum_up = lax.ppermute(packed(sum_low + unpacked(far_up)), RING, UP)
    sum_down = lax.ppermute(packed(sum_high + unpacked(far_down)), RING, DOWN)
    found = given(own, 0, width)
    low = found[:, :half] + dot(own[1], weight[:, :half])
    high = found[:, half:] + dot(own[1], weight[:, half:])
    low, high = lax.optimization_barrier((low, high))
    low = low + unpacked(near_down)
    high = high + unpacked(near_up)
    low, high = lax.optimization_barrier((low, high))
    low = low + unpacked(sum_up)
    high = high + unpacked(sum_down)

    first = vocab_index * width
    ids = first + lax.broadcasted_iota(jnp.int32, low.shape, 1)
    peak = jnp.maximum(jnp.max(low, axis=1), jnp.max(high, axis=1))
    mass = jnp.sum(jnp.exp(low - peak[:, None]), axis=1) + jnp.sum(
        jnp.exp(high - peak[:, None]), axis=1
    )
    picked = jnp.sum(jnp.where(ids == labels[:, None], low, 0.0), axis=1) + jnp.sum(
        jnp.where(ids + half == labels[:, None], high, 0.0), axis=1
    )

    shape = (peak.shape[0], 8, 2 * deal)
    row, owner, place = (lax.broadcasted_iota(jnp.int32, shape, d) for d in range(3))
    token = targets.shape[1] * owner + 4 * deal * (place // deal) + place % deal
    hit = token + deal * ring == token_of(row)
    peak, mass, picked = (
        jnp.sum(jnp.where(hit, value[:, None, None], 0.0), axis=0)
        for value in (peak, mass, picked)
    )
    stats = jnp.stack([peak, mass, picked], axis=1)
    stats = jnp.broadcast_to(stats, (16, *stats.shape)).reshape(128, *stats.shape[1:])
    stats = lax.all_to_all(stats, EVERY, split_axis=0, concat_axis=0, tiled=True)
    stats = stats.reshape(16, 4, 2, *stats.shape[1:])
    peaks, masses, picks = stats[:, :, :, 0], stats[:, :, :, 1], stats[:, :, :, 2]
    top = jnp.max(peaks, axis=0)
    total = jnp.sum(masses * jnp.exp(peaks - top), axis=0)
    log_norm = top + jnp.log(total)
    entropy = log_norm - jnp.sum(picks, axis=0)

    shape = (*entropy.shape, targets.shape[1])
    source, _, place, wanted = (lax.broadcasted_iota(jnp.int32, shape, d) for d in range(4))
    hit = 4 * deal * (place // deal) + deal * source + place % deal == wanted

    def in_order(values):
        return jnp.sum(jnp.where(hit, values[..., None], 0.0), axis=(0, 2))

    return in_order(entropy), in_order(log_norm * log_norm)


def solution(mesh):
    finer = Mesh(mesh.devices.reshape(4, 4, 4, 2), EVERY)
    return jax.shard_map(
        losses,
        mesh=finer,
        in_specs=(P(None, VOCAB, HID), P(HID, VOCAB), P(None, HID)),
        out_specs=(P(None, HID), P(None, HID)),
        check_vma=False,
    )
```

```python
import jax
import jax.numpy as jnp
from jax import lax
from jax.experimental import pallas as pl
from jax.experimental.pallas import tpu as pltpu
from jax.sharding import Mesh
from jax.sharding import PartitionSpec as P

VOCAB = ("vocab_0", "vocab_1")
HID = ("hid_0", "hid_1")
EVERY = (*VOCAB, *HID)
RING = "hid_0"
CORE = "hid_1"
UP = [(i, (i + 1) % 4) for i in range(4)]
DOWN = [(i, (i - 1) % 4) for i in range(4)]
ACROSS = [(i, (i + 2) % 4) for i in range(4)]
SWAP = [(0, 1), (1, 0)]
WAYS = (UP, DOWN, ACROSS)
OFFSETS = (0, 3, 1, 2)
SCALE = 1.0 / 16.0


def packed(partial):
    return (partial * SCALE).astype(jnp.float16)


def unpacked(message):
    return message.astype(jnp.float32) * (1.0 / SCALE)


def dot(rows, columns):
    return jnp.dot(rows, columns, preferred_element_type=jnp.float32)


def after(value, *earlier):
    return lax.optimization_barrier((value, *earlier))[0]


def take(array, index, axis):
    return lax.dynamic_index_in_dim(array, index, axis, False)


def offset(k):
    return jnp.where(k == 0, 0, jnp.where(k == 1, 3, k - 1))


def fetch(given, kept, done):
    copy = pltpu.make_async_copy(given, kept, done)
    copy.start()
    copy.wait()


def resident(array):
    return pl.pallas_call(
        fetch,
        out_shape=pltpu.VMEM(array.shape, array.dtype),
        in_specs=[pl.BlockSpec(memory_space=pltpu.HBM)],
        out_specs=pl.BlockSpec(memory_space=pltpu.VMEM),
        scratch_shapes=[pltpu.SemaphoreType.DMA],
        compiler_params=pltpu.CompilerParams(vmem_limit_bytes=40 << 20),
        name="resident",
    )(array)


def losses(hidden, head_weight, targets):
    ring = lax.axis_index(RING)
    core = lax.axis_index(CORE)
    vocab_index = lax.axis_index(VOCAB)
    width = head_weight.shape[1]
    half = width // 2
    deal = hidden.shape[1] // 4
    weight = resident(head_weight)

    dealt = hidden.reshape(2, 4, deal, hidden.shape[2])
    dealt = jnp.stack([take(dealt, 1 - core, 0), take(dealt, core, 0)])
    dealt = jnp.stack([take(dealt, (ring + k) % 4, 1) for k in (2, 1, 3, 0)], axis=1)

    def token_of(row):
        plane_at = lax.rem(lax.axis_index(VOCAB[0]) + offset(row // (4 * deal)), 4)
        line_at = lax.rem(lax.axis_index(VOCAB[1]) + offset(row // deal % 4), 4)
        return 4 * deal * (4 * plane_at + line_at) + deal * ring + row % deal

    mine = lax.dynamic_slice_in_dim(targets, core, 1)
    mate = lax.dynamic_slice_in_dim(targets, 1 - core, 1)
    pair = jnp.concatenate([mine, lax.ppermute(mate, CORE, SWAP)])
    labels = 0
    for k, way in enumerate((None, *WAYS)):
        piece = pair if way is None else lax.ppermute(pair, RING, way)
        shape = (16 * deal, *piece.shape)
        side, place = (lax.broadcasted_iota(jnp.int32, shape, d) for d in (1, 2))
        owner = 2 * lax.rem(ring + OFFSETS[k], 4) + jnp.where(side == 0, core, 1 - core)
        wanted = token_of(lax.broadcasted_iota(jnp.int32, shape, 0))
        hit = owner * piece.shape[1] + place == wanted
        labels = labels + jnp.sum(jnp.where(hit, piece, 0), axis=(1, 2))

    def around(block, axis):
        return [lax.ppermute(block, axis, way) for way in WAYS]

    plane = [dealt, *around(dealt, VOCAB[1])]
    plane = jnp.stack(plane, axis=2).reshape(2, 4, 4 * deal, hidden.shape[2])
    far = around(plane[:, 0], VOCAB[0])
    rest = around(plane[:, 1:3], VOCAB[0])
    last = around(plane[:, 3], VOCAB[0])

    def given(rows, lo, size):
        partial = dot(rows[0], weight[:, lo : lo + size])
        return lax.ppermute(partial, CORE, SWAP)

    def both(rows, lo):
        found = given(rows, lo, half)
        return found + dot(rows[1], weight[:, lo : lo + half])

    far = jnp.concatenate([plane[:, 0], *far], axis=1)
    far_up = packed(both(far, 0))
    far_down = packed(both(far, half))
    rest = jnp.concatenate([plane[:, 1:3], *rest], axis=2)
    rest = after(rest, far_up, far_down)
    near_up = packed(both(rest[:, 0], half))
    near_down = packed(both(rest[:, 1], 0))
    rest = after(rest, near_up, near_down)
    sum_low = both(rest[:, 0], 0)
    sum_high = both(rest[:, 1], half)
    own = jnp.concatenate([plane[:, 3], *last], axis=1)
    own = after(own, sum_low, sum_high)
    far_up = lax.ppermute(far_up, RING, UP)
    far_down = lax.ppermute(far_down, RING, DOWN)
    near_up = lax.ppermute(near_up, RING, UP)
    near_down = lax.ppermute(near_down, RING, DOWN)
    sum_low, sum_high = lax.optimization_barrier((sum_low, sum_high))
    sum_up = lax.ppermute(packed(sum_low + unpacked(far_up)), RING, UP)
    sum_down = lax.ppermute(packed(sum_high + unpacked(far_down)), RING, DOWN)
    found = given(own, 0, width)
    both_halves = found + dot(own[1], weight)
    low, high = both_halves[:, :half], both_halves[:, half:]
    low, high = lax.optimization_barrier((low, high))
    low = low + unpacked(near_down)
    high = high + unpacked(near_up)
    low, high = lax.optimization_barrier((low, high))
    low = low + unpacked(sum_up)
    high = high + unpacked(sum_down)

    first = vocab_index * width
    ids = first + lax.broadcasted_iota(jnp.int32, low.shape, 1)
    peak = jnp.maximum(jnp.max(low, axis=1), jnp.max(high, axis=1))
    mass = jnp.sum(jnp.exp(low - peak[:, None]), axis=1) + jnp.sum(
        jnp.exp(high - peak[:, None]), axis=1
    )
    picked = jnp.sum(jnp.where(ids == labels[:, None], low, 0.0), axis=1) + jnp.sum(
        jnp.where(ids + half == labels[:, None], high, 0.0), axis=1
    )

    shape = (peak.shape[0], 8, 2 * deal)
    row, owner, place = (lax.broadcasted_iota(jnp.int32, shape, d) for d in range(3))
    token = targets.shape[1] * owner + 4 * deal * (place // deal) + place % deal
    hit = token + deal * ring == token_of(row)
    peak, mass, picked = (
        jnp.sum(jnp.where(hit, value[:, None, None], 0.0), axis=0)
        for value in (peak, mass, picked)
    )
    stats = jnp.concatenate([peak, mass, picked], axis=1)
    stats = stats.reshape(8, 1, -1)
    stats = jnp.broadcast_to(stats, (16, *stats.shape)).reshape(128, 1, -1)
    stats = lax.all_to_all(stats, EVERY, split_axis=0, concat_axis=0, tiled=True)
    stats = stats.reshape(16, 4, 2, -1)
    peaks, masses, picks = jnp.split(stats, 3, axis=-1)
    top = jnp.max(peaks, axis=0)
    total = jnp.sum(masses * jnp.exp(peaks - top), axis=0)
    log_norm = top + jnp.log(total)
    entropy = log_norm - jnp.sum(picks, axis=0)

    shape = (*entropy.shape, targets.shape[1])
    source, _, place, wanted = (lax.broadcasted_iota(jnp.int32, shape, d) for d in range(4))
    hit = 4 * deal * (place // deal) + deal * source + place % deal == wanted

    def in_order(values):
        return jnp.sum(jnp.where(hit, values[..., None], 0.0), axis=(0, 2))

    return in_order(entropy), in_order(log_norm * log_norm)


def solution(mesh):
    finer = Mesh(mesh.devices.reshape(4, 4, 4, 2), EVERY)
    return jax.shard_map(
        losses,
        mesh=finer,
        in_specs=(P(None, VOCAB, HID), P(HID, VOCAB), P(None, HID)),
        out_specs=(P(None, HID), P(None, HID)),
        check_vma=False,
    )
```

```python
import jax
import jax.numpy as jnp
from jax import lax
from jax.experimental import pallas as pl
from jax.experimental.pallas import tpu as pltpu
from jax.sharding import Mesh
from jax.sharding import PartitionSpec as P

VOCAB = ("vocab_0", "vocab_1")
HID = ("hid_0", "hid_1")
EVERY = (*VOCAB, *HID)
RING = "hid_0"
CORE = "hid_1"
UP = [(i, (i + 1) % 4) for i in range(4)]
DOWN = [(i, (i - 1) % 4) for i in range(4)]
ACROSS = [(i, (i + 2) % 4) for i in range(4)]
SWAP = [(0, 1), (1, 0)]
BESIDE = [(i, i ^ 1) for i in range(4)]
BETWEEN = [(i, 3 - i) for i in range(4)]
WAYS = (UP, DOWN, ACROSS)
OFFSETS = (0, 3, 1, 2)
SCALE = 1.0 / 16.0


def packed(partial):
    return (partial * SCALE).astype(jnp.float16)


def unpacked(message):
    return message.astype(jnp.float32) * (1.0 / SCALE)


def dot(rows, columns):
    return jnp.dot(rows, columns, preferred_element_type=jnp.float32)


def after(value, *earlier):
    return lax.optimization_barrier((value, *earlier))[0]


def take(array, index, axis):
    return lax.dynamic_index_in_dim(array, index, axis, False)


def offset(k):
    return jnp.where(k == 0, 0, jnp.where(k == 1, 3, k - 1))


def met(here, k):
    beside = lax.bitwise_xor(here, 1)
    return jnp.where(k == 0, here, jnp.where(k == 1, beside, jnp.where(k == 2, 3 - here, 3 - beside)))


def fetch(given, kept, done):
    copy = pltpu.make_async_copy(given, kept, done)
    copy.start()
    copy.wait()


def resident(array):
    return pl.pallas_call(
        fetch,
        out_shape=pltpu.VMEM(array.shape, array.dtype),
        in_specs=[pl.BlockSpec(memory_space=pltpu.HBM)],
        out_specs=pl.BlockSpec(memory_space=pltpu.VMEM),
        scratch_shapes=[pltpu.SemaphoreType.DMA],
        compiler_params=pltpu.CompilerParams(vmem_limit_bytes=40 << 20),
        name="resident",
    )(array)


def losses(hidden, head_weight, targets):
    ring = lax.axis_index(RING)
    core = lax.axis_index(CORE)
    vocab_index = lax.axis_index(VOCAB)
    width = head_weight.shape[1]
    half = width // 2 + 128
    deal = hidden.shape[1] // 4
    weight = resident(head_weight)

    dealt = hidden.reshape(2, 4, deal, hidden.shape[2])
    dealt = jnp.stack([take(dealt, 1 - core, 0), take(dealt, core, 0)])
    dealt = jnp.stack([take(dealt, (ring + k) % 4, 1) for k in (2, 1, 3, 0)], axis=1)

    def token_of(row):
        plane_at = met(lax.axis_index(VOCAB[0]), row // (4 * deal))
        line_at = lax.rem(lax.axis_index(VOCAB[1]) + offset(row // deal % 4), 4)
        return 4 * deal * (4 * plane_at + line_at) + deal * ring + row % deal

    mine = lax.dynamic_slice_in_dim(targets, core, 1)
    mate = lax.dynamic_slice_in_dim(targets, 1 - core, 1)
    pair = jnp.concatenate([mine, lax.ppermute(mate, CORE, SWAP)])
    labels = 0
    for k, way in enumerate((None, *WAYS)):
        piece = pair if way is None else lax.ppermute(pair, RING, way)
        shape = (16 * deal, *piece.shape)
        side, place = (lax.broadcasted_iota(jnp.int32, shape, d) for d in (1, 2))
        owner = 2 * lax.rem(ring + OFFSETS[k], 4) + jnp.where(side == 0, core, 1 - core)
        wanted = token_of(lax.broadcasted_iota(jnp.int32, shape, 0))
        hit = owner * piece.shape[1] + place == wanted
        labels = labels + jnp.sum(jnp.where(hit, piece, 0), axis=(1, 2))

    def around(block, axis):
        return [lax.ppermute(block, axis, way) for way in WAYS]

    plane = [dealt, *around(dealt, VOCAB[1])]
    plane = jnp.stack(plane, axis=2).reshape(2, 4, 4 * deal, hidden.shape[2])
    back, ahead, away = around(plane[:, 0], VOCAB[0])
    even = lax.axis_index(VOCAB[0]) % 2 == 0
    beside, between = jnp.where(even, ahead, back), jnp.where(even, back, ahead)
    far = jnp.concatenate([plane[:, 0], beside, between, away], axis=1)

    one, three = plane[:, 1], plane[:, 2]
    one = jnp.concatenate([one, lax.ppermute(one, VOCAB[0], BESIDE)], axis=1)
    three = jnp.concatenate([three, lax.ppermute(three, VOCAB[0], BETWEEN)], axis=1)
    more_one = lax.ppermute(one, VOCAB[0], BETWEEN)
    more_three = lax.ppermute(three, VOCAB[0], BESIDE)
    own = plane[:, 3]
    own = jnp.concatenate([own, lax.ppermute(own, VOCAB[0], BESIDE)], axis=1)
    own = jnp.concatenate([own, lax.ppermute(own, VOCAB[0], BETWEEN)], axis=1)

    def given(rows, lo, size):
        partial = packed(dot(rows[0], weight[:, lo : lo + size]))
        return unpacked(lax.ppermute(partial, CORE, SWAP))

    def both(rows, lo):
        size = half if lo == 0 else width - half
        found = given(rows, lo, size)
        return found + dot(rows[1], weight[:, lo : lo + size])

    far_up = packed(both(far, 0))
    far_down = packed(both(far, half))
    one = jnp.concatenate([one, more_one], axis=1)
    each = jnp.split(three, 2, axis=1), jnp.split(more_three, 2, axis=1)
    three = jnp.concatenate([each[0][0], each[1][0], each[0][1], each[1][1]], axis=1)
    one, three, *_ = lax.optimization_barrier((one, three, far_up, far_down))
    near_up = packed(both(one, half))
    near_down = packed(both(three, 0))
    one, three, *_ = lax.optimization_barrier((one, three, near_up, near_down))
    sum_low = both(one, 0)
    sum_high = both(three, half)
    own = after(own, sum_low, sum_high)
    far_up = lax.ppermute(far_up, RING, UP)
    far_down = lax.ppermute(far_down, RING, DOWN)
    near_up = lax.ppermute(near_up, RING, UP)
    near_down = lax.ppermute(near_down, RING, DOWN)
    sum_low, sum_high = lax.optimization_barrier((sum_low, sum_high))
    sum_up = lax.ppermute(packed(sum_low + unpacked(far_up)), RING, UP)
    sum_down = lax.ppermute(packed(sum_high + unpacked(far_down)), RING, DOWN)
    found = given(own, 0, width)
    both_halves = found + dot(own[1], weight)
    low, high = both_halves[:, :half], both_halves[:, half:]
    low, high = lax.optimization_barrier((low, high))
    low = low + unpacked(near_down)
    high = high + unpacked(near_up)
    low, high = lax.optimization_barrier((low, high))
    low = low + unpacked(sum_up)
    high = high + unpacked(sum_down)

    def statistics(logits, first):
        ids = first + lax.broadcasted_iota(jnp.int32, logits.shape, 1)
        peak = jnp.max(logits, axis=1)
        mass = jnp.sum(jnp.exp(logits - peak[:, None]), axis=1)
        return peak, mass, jnp.sum(jnp.where(ids == labels[:, None], logits, 0.0), axis=1)

    first = vocab_index * width
    low_peak, low_mass, low_picked = statistics(low, first)
    high_peak, high_mass, high_picked = statistics(high, first + half)
    peak = jnp.maximum(low_peak, high_peak)
    mass = low_mass * jnp.exp(low_peak - peak) + high_mass * jnp.exp(high_peak - peak)
    picked = low_picked + high_picked

    shape = (peak.shape[0], 8, 2 * deal)
    row, owner, place = (lax.broadcasted_iota(jnp.int32, shape, d) for d in range(3))
    token = targets.shape[1] * owner + 4 * deal * (place // deal) + place % deal
    hit = token + deal * ring == token_of(row)
    peak, mass, picked = (
        jnp.sum(jnp.where(hit, value[:, None, None], 0.0), axis=0)
        for value in (peak, mass, picked)
    )
    stats = jnp.concatenate([peak, mass, picked], axis=1)
    stats = stats.reshape(8, 1, -1)
    stats = jnp.broadcast_to(stats, (16, *stats.shape)).reshape(128, 1, -1)
    stats = lax.all_to_all(stats, EVERY, split_axis=0, concat_axis=0, tiled=True)
    stats = stats.reshape(16, 4, 2, -1)
    peaks, masses, picks = jnp.split(stats, 3, axis=-1)
    top = jnp.max(peaks, axis=0)
    total = jnp.sum(masses * jnp.exp(peaks - top), axis=0)
    log_norm = top + jnp.log(total)
    entropy = log_norm - jnp.sum(picks, axis=0)

    shape = (*entropy.shape, targets.shape[1])
    source, _, place, wanted = (lax.broadcasted_iota(jnp.int32, shape, d) for d in range(4))
    hit = 4 * deal * (place // deal) + deal * source + place % deal == wanted

    def in_order(values):
        return jnp.sum(jnp.where(hit, values[..., None], 0.0), axis=(0, 2))

    return in_order(entropy), in_order(log_norm * log_norm)


def solution(mesh):
    finer = Mesh(mesh.devices.reshape(4, 4, 4, 2), EVERY)
    return jax.shard_map(
        losses,
        mesh=finer,
        in_specs=(P(None, VOCAB, HID), P(HID, VOCAB), P(None, HID)),
        out_specs=(P(None, HID), P(None, HID)),
        check_vma=False,
    )
```
